32 devices in a mesh: groups: 2 (over y), rows: 4 (over z), keys: 2 (over x), heads: 2 (over core).
Axes of the slice: x: 2, y: 2, z: 4, core: 2. Of those that a mesh axis runs over, the one named last changes fastest.
Arguments:
- pair: bfloat16 [1024, 512, 128], P(('groups', 'rows'), 'keys'), parts along dimension 0, may hold values from -6 to 6
- seq_length: int32 [2], P('groups'), parts along dimension 0, may hold values from 257 to 512
- tile_counts: int32 [1024, 4], P(('groups', 'rows')), parts along dimension 0, may hold values from 0 to 128, as said below
- ln_gain: float32 [128], replicated, may hold values from 0.5 to 1.5
- w_query: bfloat16 [128, 128], P(None, 'heads'), may hold values from -8 to 8
- w_key: bfloat16 [128, 128], P(None, 'heads'), may hold values from -0.5 to 0.5
- w_value: bfloat16 [128, 128], P(None, 'heads'), may hold values from -0.5 to 0.5
- w_gate: bfloat16 [128, 128], P(None, 'heads'), may hold values from -0.5 to 0.5
- w_bias: bfloat16 [128, 4], P(None, 'heads'), may hold values from -1.5 to 1.5
- w_out: bfloat16 [128, 128], replicated, may hold values from -2 to 2
Outputs:
- update: bfloat16 [1024, 512, 128], P(('groups', 'rows'), ('keys', 'heads')), parts along dimension 0
The draws below stay inside these ranges and needn't reach their ends.
There are 2 independent parts, one for each index of `groups`. The reference program is written for one: setup_inputs(seed, part) draws one part's arguments, and reference() takes and returns one part's arrays. A program takes and returns all parts, laid end to end along the dimension named above; an argument that names none is the same for every part. Nothing has to cross between parts.
Inputs may be any that keep to these rules, and one draw needn't show every extreme that they name: `tile_counts`: for each row and each tile of 128 keys, how many of the tile's leading keys are valid; some rows have no valid key at all.
All inputs are finite; a program needn't handle non-finite values.
Results may differ from the reference program's by a relative error of at most 0.03.
The reference program's roundings to bfloat16 on the way count: a program that leaves them out, or rounds other values in their place, can miss the bound.
Values may be sent and summed in bfloat16 or wider, within the bound.
A program may use at most 192 MiB of HBM per device.

```python
import jax
import jax.numpy as jnp
from jax import lax

C = 128
HEADS = 4
HEAD_DIM = 32
TILE = 128
L = 512


def draw_tile_counts(key, part):
    first, second = jax.random.split(jax.random.fold_in(key, 11))
    counts = jax.random.randint(first, (L, L // TILE), 0, TILE + 1)
    keeper = jax.random.randint(second, (L, 1), 0, 8) > 0
    return jnp.where(keeper, counts, 0).astype(jnp.int32)


def draw_w_query(key, part):
    inner = jax.random.fold_in(key, 23)
    drawn = jnp.clip(jax.random.normal(inner, (C, HEADS * HEAD_DIM), jnp.float32), -4.0, 4.0) * C ** (-0.5)
    return drawn.astype(jnp.bfloat16)


def block_levels(stream_key, extent, cuts, least, top_value):
    def one(position, blocks):
        heights = jax.random.uniform(jax.random.fold_in(jax.random.fold_in(stream_key, 6), position), (blocks,), jnp.float32, least / len(cuts), top_value / len(cuts))
        return jnp.repeat(jnp.exp(heights), extent[position] // blocks).reshape((-1,) + (1,) * (len(extent) - position - 1))

    level = one(*cuts[0])
    for cut in cuts[1:]:
        level = level * one(*cut)
    return level


def centred(rng, extent, deviation, reach, cuts=(), kind=jnp.bfloat16):
    values = deviation * jax.random.normal(rng, extent, jnp.float32)
    if cuts:
        values = values * block_levels(rng, extent, cuts, -0.22, 0.18)
    return jnp.clip(values, -reach, reach).astype(kind)


def setup_inputs(seed: int = 0, part: int = 0) -> dict:
    streams_of = jax.random.split(jax.random.key(seed), 11)
    part_splits = jax.random.split(jax.random.fold_in(streams_of[10], part), 11)
    pair = centred(part_splits[0], (L, L, C), 1.0, 6.0, ((0, 4), (1, 2)))
    seq_length = jax.random.randint(part_splits[1], (1,), L // 2 + 1, L + 1).astype(jnp.int32)
    tile_counts = draw_tile_counts(jax.random.fold_in(jax.random.fold_in(streams_of[10], part), 71), part)
    ln_gain = jnp.clip(1.0 + 0.1 * jax.random.normal(streams_of[3], (C,), jnp.float32), 0.5, 1.5)
    w_query = draw_w_query(jax.random.fold_in(streams_of[10], 71), part)
    w_key = centred(streams_of[5], (C, HEADS * HEAD_DIM), C ** -0.5, 0.5, ((1, 2),))
    w_value = centred(streams_of[6], (C, HEADS * HEAD_DIM), C ** -0.5, 0.5, ((1, 2),))
    w_gate = centred(streams_of[7], (C, HEADS * HEAD_DIM), C ** -0.5, 0.5, ((1, 2),))
    w_bias = centred(streams_of[8], (C, HEADS), (C // 8) ** -0.5, 1.5, ((1, 2),))
    w_out = centred(streams_of[9], (HEADS * HEAD_DIM, C), (HEADS * HEAD_DIM // 16) ** -0.5, 2.0)
    return dict(pair=pair, seq_length=seq_length, tile_counts=tile_counts, ln_gain=ln_gain, w_query=w_query, w_key=w_key, w_value=w_value, w_gate=w_gate, w_bias=w_bias, w_out=w_out)


norm_epsilon = 1e-05
masked_score = -1e+30

def layer_norm(values, gain):
    center = values - lax.optimization_barrier(jnp.mean(values, axis=-1, keepdims=True))
    spread = lax.optimization_barrier(jnp.mean(center * center, axis=-1, keepdims=True))
    return center * lax.rsqrt(spread + norm_epsilon) * gain

def reference(pair, seq_length, tile_counts, ln_gain, w_query, w_key, w_value, w_gate, w_bias, w_out):
    width = HEADS * HEAD_DIM
    normed = layer_norm(pair.astype(jnp.float32), ln_gain).astype(jnp.bfloat16)
    flat = normed.reshape(L * L, C)
    queries = (jnp.dot(flat, w_query, preferred_element_type=jnp.float32) * HEAD_DIM ** (-0.5)).astype(jnp.bfloat16).reshape(L, L, HEADS, HEAD_DIM)
    keys_all = jnp.dot(flat, w_key, preferred_element_type=jnp.float32).astype(jnp.bfloat16).reshape(L, L, HEADS, HEAD_DIM)
    values_all = jnp.dot(flat, w_value, preferred_element_type=jnp.float32).astype(jnp.bfloat16).reshape(L, L, HEADS, HEAD_DIM)
    gate_act = jax.nn.sigmoid(jnp.dot(flat, w_gate, preferred_element_type=jnp.float32)).reshape(L, L, width)
    pair_bias = jnp.einsum('jkc,ch->hjk', normed.astype(jnp.float32), w_bias.astype(jnp.float32))
    positions = jnp.arange(L, dtype=jnp.int32)
    allowed = (positions[None, :] < seq_length[0]) & ((positions % TILE)[None, :] < jnp.repeat(tile_counts, TILE, axis=1))

    def one_row(operands):
        row_queries, row_keys, row_values, row_allowed = operands
        shown = row_allowed[None, None, :]
        scores = jnp.einsum('jhd,khd->hjk', row_queries.astype(jnp.float32), row_keys.astype(jnp.float32)) + pair_bias
        scores = jnp.where(shown, scores, masked_score)
        row_max = lax.optimization_barrier(jnp.max(scores, axis=-1, keepdims=True))
        weights = jnp.where(shown, jnp.exp(scores - row_max), 0.0)
        row_sum = lax.optimization_barrier(jnp.sum(weights, axis=-1))
        rounded = lax.optimization_barrier(weights.astype(jnp.bfloat16)).astype(jnp.float32)
        mixed = jnp.einsum('hjk,khd->jhd', rounded, row_values.astype(jnp.float32))
        denom = jnp.maximum(row_sum, 1.0)
        return (mixed / jnp.transpose(denom)[:, :, None]).astype(jnp.bfloat16)
    attended = lax.map(one_row, (queries, keys_all, values_all, allowed))
    attended = lax.optimization_barrier(attended.reshape(L, L, width)).astype(jnp.float32)
    gated = (gate_act * attended).astype(jnp.bfloat16)
    update = jnp.dot(gated.reshape(L * L, width), w_out, preferred_element_type=jnp.float32)
    return update.astype(jnp.bfloat16).reshape(L, L, C)
```

```python
import functools
import math

import jax
import jax.numpy as jnp
from jax import lax
from jax.experimental import pallas as pl
from jax.experimental.pallas import tpu as pltpu
from jax.sharding import PartitionSpec as P

HEAD_DIM = 32
TILE = 128
LOG2E = math.log2(math.e)
ROWS_OF_64 = (20, 24, 20)

norm_epsilon = 1e-05
masked_score = -1e30


def layer_norm(values, gain):
    center = values - jnp.mean(values, axis=-1, keepdims=True)
    spread = jnp.mean(center * center, axis=-1, keepdims=True)
    return center * lax.rsqrt(spread + norm_epsilon) * gain


def dot_nt(a, b):
    return lax.dot_general(a, b, (((1,), (1,)), ((), ())), preferred_element_type=jnp.float32)


def dot_tn(a, b):
    return lax.dot_general(a, b, (((0,), (0,)), ((), ())), preferred_element_type=jnp.float32)


def bias_kernel(_, pair_ref, gain_ref, w_ref, out_ref, by_row):
    rows, cols, channels = pair_ref.shape
    padded = by_row.shape[1]
    step = pl.program_id(0)
    flat = pair_ref[...].reshape(rows * cols, channels).astype(jnp.float32)
    normed = layer_norm(flat, gain_ref[...]).astype(jnp.bfloat16)
    found = dot_nt(w_ref[...], normed)
    for r in range(rows):
        by_row[step * rows + r] = found[:padded, r * cols : (r + 1) * cols]

    @pl.when(step == pl.num_programs(0) - 1)
    def _():
        for h in range(out_ref.shape[0]):
            out_ref[h] = (by_row[:, h, :] * LOG2E).astype(jnp.bfloat16)


def pair_bias_part(pair, core, cols, gain, w_bias_t, heads):
    rows, _, channels = pair.shape
    block = min(rows, 16)
    padded = -(-heads // 8) * 8
    return pl.pallas_call(
        bias_kernel,
        grid_spec=pltpu.PrefetchScalarGridSpec(
            num_scalar_prefetch=1,
            grid=(rows // block,),
            in_specs=[
                pl.BlockSpec((block, cols, channels), lambda r, which: (r, which[0], 0)),
                pl.BlockSpec((1, channels), lambda r, which: (0, 0)),
                pl.BlockSpec(w_bias_t.shape, lambda r, which: (0, 0)),
            ],
            out_specs=pl.BlockSpec((heads, rows, cols), lambda r, which: (0, 0, 0)),
            scratch_shapes=[pltpu.VMEM((rows, padded, cols), jnp.float32)],
        ),
        out_shape=jax.ShapeDtypeStruct((heads, rows, cols), jnp.bfloat16),
        cost_estimate=pl.CostEstimate(
            flops=rows * cols * channels * 200, bytes_accessed=rows * cols * channels * 2,
            transcendentals=0,
        ),
        name="pair_bias",
    )(core, pair, gain, w_bias_t)


def row_limits(counts_ref, row, seq, parts, tiles):
    limits = []
    for part in parts:
        for t in range(tiles):
            g = part * tiles + t
            limits.append(jnp.minimum(counts_ref[row, g], seq - g * TILE))
    return limits, functools.reduce(jnp.maximum, limits)


def own_kernel(info_ref, seq_ref, counts_ref, pair_ref, gain_ref, w_ref, kv_ref, q_ref, gate_ref, *, parts):
    rows, cols, channels = pair_ref.shape
    step = pl.program_id(0)
    order = [info_ref[1 + p] for p in range(parts)]
    most = [
        row_limits(counts_ref, step * rows + r, seq_ref[0], order, cols // TILE)[1]
        for r in range(rows)
    ]

    @pl.when(functools.reduce(jnp.maximum, most) > 0)
    def _():
        flat = pair_ref[...].reshape(rows * cols, channels).astype(jnp.float32)
        normed = layer_norm(flat, gain_ref[...]).astype(jnp.bfloat16)
        found = jnp.dot(normed, w_ref[...], preferred_element_type=jnp.float32)
        found = found.reshape(rows, cols, 4 * channels)
        kv_ref[...] = found[:, :, : 2 * channels].astype(jnp.bfloat16)
        scale = HEAD_DIM ** -0.5 * LOG2E
        q_ref[...] = (found[:, :, 2 * channels : 3 * channels] * scale).astype(jnp.bfloat16)
        gate_ref[...] = jax.nn.sigmoid(found[:, :, 3 * channels :])


def own_rows(info, seq_length, counts, pair, gain, w, parts):
    _, cols, channels = pair.shape
    rows = counts.shape[0]
    block = 2 if rows % 2 == 0 else 1
    steps = rows // block
    spec = lambda width: pl.BlockSpec((block, cols, width), lambda r, *_: (r, 0, 0))
    return pl.pallas_call(
        functools.partial(own_kernel, parts=parts),
        grid_spec=pltpu.PrefetchScalarGridSpec(
            num_scalar_prefetch=3,
            grid=(steps,),
            in_specs=[
                pl.BlockSpec((block, cols, channels), lambda r, info, *_: (info[0] * steps + r, 0, 0)),
                pl.BlockSpec(gain.shape, lambda r, *_: (0, 0)),
                pl.BlockSpec(w.shape, lambda r, *_: (0, 0)),
            ],
            out_specs=[spec(2 * channels), spec(channels), spec(channels)],
        ),
        out_shape=[
            jax.ShapeDtypeStruct((rows, cols, 2 * channels), jnp.bfloat16),
            jax.ShapeDtypeStruct((rows, cols, channels), jnp.bfloat16),
            jax.ShapeDtypeStruct((rows, cols, channels), jnp.float32),
        ],
        cost_estimate=pl.CostEstimate(
            flops=rows * cols * channels * 8000, bytes_accessed=rows * cols * channels * 12,
            transcendentals=rows * cols * channels,
        ),
        name="own_rows",
    )(info, seq_length, counts, pair, gain, w)


def attention_kernel(info_ref, seq_ref, counts_ref, *refs, others, base, rows):
    kv_ref, q_ref, gate_ref = refs[:3]
    pairs = refs[3 : 3 + others]
    gain_ref, wk_ref, wo_ref, blocks_ref = refs[3 + others : 7 + others]
    mine_ref, theirs_ref, bias_ref = refs[-9:-6]
    slots = (refs[-6:-3], refs[-3:])
    _, cols, channels = q_ref.shape
    heads = bias_ref.shape[0]
    step = pl.program_id(0)
    tiles = cols // TILE
    length = (1 + others) * cols
    width = mine_ref.shape[1]
    shards = cols // width
    core = info_ref[0]
    order = [info_ref[1 + p] for p in range(1 + others)]
    seq = seq_ref[0]
    coming, most = row_limits(counts_ref, base + jnp.minimum(step, rows - 1), seq, order, tiles)
    _, least = row_limits(counts_ref, base + jnp.maximum(step - 1, 0), seq, order, tiles)
    project_now = (most > 0) & (step < rows)
    attend_now = (least > 0) & (step > 0)
    even = lax.rem(step, 2) == 0

    @pl.when(step == 0)
    def _():
        lane = lax.broadcasted_iota(jnp.int32, (cols, channels), 1)
        for _, query_s, value_s in slots:
            for h in range(heads):
                hide = jnp.where(lane == 0, masked_score, 0.0)
                query_s[h, :, channels:] = hide.astype(jnp.bfloat16)
            value_s[:, channels:] = jnp.ones((length, channels), jnp.bfloat16)
        halves, needed, parts, _, part_rows, part_cols = blocks_ref.shape
        for n in range(needed):
            down = slice(n * part_rows, (n + 1) * part_rows)
            for p in range(parts):
                for c in range(halves):
                    first = p * cols + c * part_cols
                    block = blocks_ref[c, n, p].astype(jnp.float32)
                    bias_ref[:, down, first : first + part_cols] = block

    def project(slot):
        key_s, query_s, value_s = slot
        lane = lax.broadcasted_iota(jnp.int32, (cols, channels), 1)
        depth = lax.broadcasted_iota(jnp.int32, (TILE, channels), 0)
        q = q_ref[0]
        for h in range(heads):
            mine = (lane >= h * HEAD_DIM) & (lane < (h + 1) * HEAD_DIM)
            query_s[h, :, :channels] = jnp.where(mine, q.astype(jnp.float32), 0.0).astype(jnp.bfloat16)
        key_s[:cols, :channels] = kv_ref[0, :, :channels]
        value_s[:cols, :channels] = kv_ref[0, :, channels:]
        for p in range(1 + others):
            for t in range(tiles):
                hidden = jnp.where(depth < coming[p * tiles + t], 0.0, 1.0).astype(jnp.bfloat16)
                first = p * cols + t * TILE
                key_s[first : first + TILE, channels:] = hidden
        for p in range(others):
            span = slice((p + 1) * cols, (p + 2) * cols)
            normed = layer_norm(pairs[p][0].astype(jnp.float32), gain_ref[...])
            kv = jnp.dot(normed.astype(jnp.bfloat16), wk_ref[...], preferred_element_type=jnp.float32)
            key_s[span, :channels] = kv[:, :channels].astype(jnp.bfloat16)
            value_s[span, :channels] = kv[:, channels:].astype(jnp.bfloat16)

    def attend(slot):
        key_s, query_s, value_s = slot
        lane = lax.broadcasted_iota(jnp.int32, (cols, channels), 1)
        stacked = query_s[...].reshape(heads * cols, 2 * channels)
        every = dot_nt(stacked, key_s[...])
        for h in range(heads):
            scores = every[h * cols : (h + 1) * cols] + bias_ref[h]
            weights = jnp.exp2(scores - jnp.max(scores, axis=-1, keepdims=True))
            mixed = jnp.dot(
                weights.astype(jnp.bfloat16), value_s[...], preferred_element_type=jnp.float32
            )
            if h == 0:
                top, low = mixed[:, :channels], mixed[:, channels:]
            else:
                later = lane >= h * HEAD_DIM
                top = jnp.where(later, mixed[:, :channels], top)
                low = jnp.where(later, mixed[:, channels:], low)
        attended = (top / jnp.maximum(low, 1.0)).astype(jnp.bfloat16).astype(jnp.float32)
        gated = (gate_ref[0] * attended).astype(jnp.bfloat16)
        update = jnp.dot(gated, wo_ref[...], preferred_element_type=jnp.float32)
        update = update.astype(jnp.bfloat16)
        for d in range(shards):
            part = update[d * width : (d + 1) * width]

            @pl.when(core == d)
            def _():
                mine_ref[0] = part

            @pl.when(core != d)
            def _():
                theirs_ref[lax.rem(d + shards - core, shards) - 1, 0] = part

    for parity in range(2):
        turn = even if parity == 0 else ~even

        @pl.when(turn & project_now & attend_now)
        def _():
            attend(slots[1 - parity])
            project(slots[parity])

        @pl.when(turn & project_now & ~attend_now)
        def _():
            project(slots[parity])

        @pl.when(turn & ~project_now & attend_now)
        def _():
            attend(slots[1 - parity])

    @pl.when(~attend_now)
    def _():
        mine_ref[...] = jnp.zeros_like(mine_ref)
        theirs_ref[...] = jnp.zeros_like(theirs_ref)


def attention(info, seq_length, counts, own, pairs, gain, wk, wo, bias, out, base, rows, shards):
    kv, q, gate = own
    _, cols, channels = q.shape
    others = len(pairs)
    heads = bias.shape[3]
    length = bias.shape[2] * cols
    all_rows = kv.shape[0]
    last = rows - 1
    whole = lambda a: pl.BlockSpec(
        a.shape, lambda r, *_: (0,) * a.ndim, pipeline_mode=pl.Buffered(1)
    )
    work = rows * heads * length * cols
    width = cols // shards
    now = lambda r: jnp.minimum(r, last)
    past = lambda r: jnp.maximum(r - 1, 0)
    bf = jnp.bfloat16
    slot = [
        pltpu.VMEM((length, 2 * channels), bf),
        pltpu.VMEM((heads, cols, 2 * channels), bf),
        pltpu.VMEM((length, 2 * channels), bf),
    ]
    return pl.pallas_call(
        functools.partial(attention_kernel, others=others, base=base, rows=rows),
        grid_spec=pltpu.PrefetchScalarGridSpec(
            num_scalar_prefetch=3,
            grid=(rows + 1,),
            in_specs=[
                pl.BlockSpec((1, cols, 2 * channels), lambda r, *_: (base + now(r), 0, 0)),
                pl.BlockSpec((1, cols, channels), lambda r, *_: (base + now(r), 0, 0)),
                pl.BlockSpec((1, cols, channels), lambda r, *_: (base + past(r), 0, 0)),
            ]
            + [pl.BlockSpec((1, cols, channels), lambda r, *_: (now(r), 0, 0))] * others
            + [whole(a) for a in (gain, wk, wo, bias)]
            + [pl.BlockSpec(memory_space=pl.ANY)] * len(out),
            out_specs=[
                pl.BlockSpec(
                    (1, width, channels),
                    lambda r, info, *_: (info[0] * all_rows + base + past(r), 0, 0),
                ),
                pl.BlockSpec((shards - 1, 1, width, channels), lambda r, *_: (0, past(r), 0, 0)),
            ],
            scratch_shapes=[pltpu.VMEM((heads, cols, length), jnp.float32)] + slot * 2,
        ),
        out_shape=[
            jax.ShapeDtypeStruct((all_rows * shards, width, channels), bf),
            jax.ShapeDtypeStruct((shards - 1, rows, width, channels), bf),
        ],
        input_output_aliases={10 + others: 0} if out else {},
        cost_estimate=pl.CostEstimate(
            flops=work * 1024, bytes_accessed=rows * length * channels * 4, transcendentals=work
        ),
        name="row_attention",
    )(info, seq_length, counts, kv, q, gate, *pairs, gain, wk, wo, bias, *out)


def split_rows(rows):
    sizes = []
    left = rows
    for part in ROWS_OF_64[:-1]:
        take = min(left, max(1, rows * part // 64))
        if take:
            sizes.append(take)
        left -= take
    if left:
        sizes.append(left)
    return sizes


def rotate(x, axis, shift):
    size = lax.axis_size(axis)
    return lax.ppermute(x, axis, [(i, (i + shift) % size) for i in range(size)])


def gather_bias(part, own, key_groups, head_groups, row_groups):
    heads, rows, span = part.shape
    x = lax.axis_index("keys")
    z = lax.axis_index("rows")
    core = lax.axis_index("heads")
    by_keys = jnp.stack([part] + [rotate(part, "keys", s) for s in range(1, key_groups)])
    needed = row_groups // key_groups
    if row_groups <= 8:
        blocks = [by_keys]
        for s in range(1, row_groups):
            pairs = []
            for zz in range(row_groups):
                xx = zz // needed
                dest = (zz + s) % row_groups
                pairs.append((zz * key_groups + xx, dest * key_groups + xx))
            blocks.append(lax.ppermute(by_keys, ("rows", "keys"), pairs))
        blocks, own = lax.optimization_barrier((blocks, own))
        blocks = jnp.stack(blocks)
        mine = [
            lax.dynamic_index_in_dim(
                blocks, lax.rem(z - (x * needed + n) + row_groups, row_groups), 0, False
            )
            for n in range(needed)
        ]
        mine = jnp.stack(mine)
    else:
        every = lax.all_gather(by_keys, "rows", axis=0)
        mine = lax.dynamic_slice_in_dim(every, x * needed, needed, 0)
    cores = jnp.stack([mine] + [rotate(mine, "heads", s) for s in range(1, head_groups)])
    ordered = [
        lax.dynamic_index_in_dim(cores, lax.rem(core - c + head_groups, head_groups), 0, False)
        for c in range(head_groups)
    ]
    return jnp.stack(ordered), own


def per_device(
    pair, seq_length, tile_counts, ln_gain, w_query, w_key, w_value, w_gate, w_bias, w_out
):
    rows_dev, cols_dev, channels = pair.shape
    key_groups = lax.axis_size("keys")
    head_groups = lax.axis_size("heads")
    row_groups = lax.axis_size("rows")
    rows = rows_dev // head_groups
    heads = w_bias.shape[1] * head_groups
    core = lax.axis_index("heads")
    x = lax.axis_index("keys")
    gain = ln_gain.reshape(1, channels)

    sizes = split_rows(rows)
    starts = [sum(sizes[:i]) for i in range(len(sizes))]

    local = jnp.concatenate([w_query, w_key, w_value, w_gate, w_bias], axis=1)
    gathered = lax.all_gather(local, "heads", axis=0)
    width = w_query.shape[1]
    big = gathered[:, :, : 4 * width].reshape(head_groups, channels, 4, width)
    big = jnp.transpose(big, (2, 1, 0, 3)).reshape(4, channels, width * head_groups)
    w_all = jnp.concatenate([big[1], big[2], big[0], big[3]], axis=1)
    bias_t = jnp.transpose(gathered[:, :, 4 * width :], (0, 2, 1)).reshape(heads, channels)
    bias_t = jnp.pad(bias_t, ((0, -heads % 16), (0, 0)))

    core_1 = jnp.reshape(core, (1,)).astype(jnp.int32)
    part = pair_bias_part(pair, core_1, cols_dev // head_groups, gain, bias_t, heads)

    arrived = []
    source = pair
    for i, (start, size) in enumerate(zip(starts, sizes)):
        if i == 1:
            source, _ = lax.optimization_barrier((pair, part))
        piece = lax.dynamic_slice_in_dim(source, core * rows + start, size, 0)
        arrived.append([rotate(piece, "keys", s) for s in range(1, key_groups)])

    counts = lax.dynamic_slice_in_dim(tile_counts, core * rows, rows, 0)
    info = jnp.stack([core] + [lax.rem(x - s + key_groups, key_groups) for s in range(key_groups)])
    info = info.astype(jnp.int32)
    own = own_rows(info, seq_length, counts, pair, gain, w_all, key_groups)
    bias, own = gather_bias(part, own, key_groups, head_groups, row_groups)

    out = []
    swapped = []
    for i, (start, size) in enumerate(zip(starts, sizes)):
        mine, theirs = attention(
            info, seq_length, counts, own, arrived[i], gain, w_all[:, : 2 * channels], w_out, bias,
            out, start, size, head_groups,
        )
        out = [mine]
        swapped.append([rotate(theirs[s - 1], "heads", s) for s in range(1, head_groups)])
    out = out[0]
    for start, others in zip(starts, swapped):
        for s, other in enumerate(others, 1):
            owner = lax.rem(core - s + head_groups, head_groups)
            out = lax.dynamic_update_slice(out, other, (owner * rows + start, 0, 0))
    return out


def solution(mesh):
    in_specs = (
        P(("groups", "rows"), "keys", None),
        P("groups"),
        P(("groups", "rows"), None),
        P(),
        P(None, "heads"),
        P(None, "heads"),
        P(None, "heads"),
        P(None, "heads"),
        P(None, "heads"),
        P(),
    )
    out_specs = P(("groups", "rows"), ("keys", "heads"), None)
    return jax.shard_map(
        per_device, mesh=mesh, in_specs=in_specs, out_specs=out_specs, check_vma=False
    )
```
